32 devices in a mesh: aa: 16 (over z, y, core), ba: 2 (over x).
Axes of the slice: x: 2, y: 2, z: 4, core: 2. Of those that a mesh axis runs over, the one named last changes fastest.
Arguments:
- inputs: bfloat16 [8192, 3584], P('aa', 'ba'), may hold values from -6 to 6
- cotangent: bfloat16 [8192, 3584], P('aa', 'ba'), may hold values from -6 to 6
- base_weight: bfloat16 [3584, 3584], P(None, 'ba'), may hold values from -0.09375 to 0.09375
- adapter_ids: int32 [8192, 1], P('aa'), may hold values from 0 to 63; in each aligned block of 512 rows (0 to 511, 512 to 1023, ...) at most 16 rows name the same one
- adapters: float32 [64, 2, 16, 3584], P('aa', None, None, 'ba'), may hold values from -0.09375 to 0.09375
- first_moment: float32 [64, 2, 16, 3584], P('aa', None, None, 'ba'), may hold values from -3 to 3
- second_moment: float32 [64, 2, 16, 3584], P('aa', None, None, 'ba'), may hold values from 0.05 to 1
Outputs:
- input_gradient: bfloat16 [8192, 3584], P('aa', 'ba')
- new_adapters: float32 [64, 2, 16, 3584], P('aa', None, None, 'ba')
- new_first: float32 [64, 2, 16, 3584], P('aa', None, None, 'ba')
- new_second: float32 [64, 2, 16, 3584], P('aa', None, None, 'ba')
- grad_norm: float32 [], replicated
The draws below stay inside these ranges and needn't reach their ends.
Inputs may be any that keep to these rules, and one draw needn't show every extreme that they name: `adapter_ids`: in the rows of one device no adapter is named by more than 16 tokens, a bound that some block reaches; every adapter is named somewhere.
All inputs are finite; a program needn't handle non-finite values.
Results may differ from the reference program's by a relative error of at most 0.0034.
Values may be sent and summed in bfloat16 or wider, within the bound.
A program may use at most 128 MiB of HBM per device.

```python
import math
import jax
import jax.numpy as jnp
import numpy as np
from jax import lax

MODEL_WIDTH = 3584
R = 16
TOK_DEV = 512
ADAPTERS = 64
MOST = 16
TOKENS = 8192
N_AA = 16


def block_scale(stream_key, dims, cuts, smallest, largest):
    factor_of = 1.0
    for dim, blocks in cuts:
        steps = jax.random.uniform(jax.random.fold_in(jax.random.fold_in(stream_key, 6), dim), (blocks,), jnp.float32, smallest / len(cuts), largest / len(cuts))
        factor_of = factor_of * jnp.repeat(jnp.exp(steps), dims[dim] // blocks).reshape((-1,) + (1,) * (len(dims) - 1 - dim))
    return factor_of


def routed_block(stream_key, own, number, rows, count, top, limit, slope):
    sequence = jax.random.permutation(stream_key, count)
    crowded, ordinary = portions_of(count, rows * top, limit, slope, True), portions_of(count, rows * top, limit, slope, False)
    places = jnp.arange(count)

    def named(sizes, rotation):
        used = int((sizes > 0).sum())
        fixed = max(1, used // 4)
        moved = fixed + (places - fixed + rotation * (used - fixed)) % max(1, count - fixed)
        return jnp.zeros((count,), jnp.int32).at[sequence[jnp.where(places < fixed, places, moved)]].set(jnp.asarray(sizes, jnp.int32))

    sizes = jnp.where(number % 4 == 0, named(crowded, number // 4), named(ordinary, number - number // 4 - 1))
    mixed = jax.random.permutation(jax.random.fold_in(own, 3), count)
    giver, taker = mixed[0:count // 2 * 2:2], mixed[1:count // 2 * 2:2]
    room = jnp.minimum(sizes[giver] - 1, limit - sizes[taker]) // 2
    room = jnp.where((giver == sequence[0]) | (taker == sequence[0]) | (sizes[taker] == 0), 0, jnp.maximum(room, 0))
    moved = jax.random.randint(jax.random.fold_in(own, 4), (count // 2,), 0, 1 << 20) % (room + 1)
    sizes = sizes.at[giver].add(-moved).at[taker].add(moved)
    members = jnp.searchsorted(jnp.cumsum(sizes), jnp.arange(rows * top), side="right").astype(jnp.int32)
    table = members.reshape(top, rows).T
    table = table[jax.random.permutation(jax.random.fold_in(own, 1), rows)]
    rotation = jax.random.randint(jax.random.fold_in(own, 2), (rows, 1), 0, top)
    return jnp.take_along_axis(table, (jnp.arange(top)[None, :] + rotation) % top, axis=1)


def portions_of(number_of, total, reach, lean, full):
    portions = [(1 << 20) // math.isqrt(standing ** lean) + 1 for standing in range(1, number_of + 1)]
    largest = reach if full else min(reach, max(-(-total // number_of), total * portions[0] // sum(portions)))
    least = 1 if total - largest >= number_of - 1 else 0
    given, spare = [largest] + [least] * (number_of - 1), total - largest - least * (number_of - 1)
    while spare > 0:
        candidates = [i for i in range(1, number_of) if given[i] < largest] or [i for i in range(1, number_of) if given[i] < reach]
        pool, left = sum([portions[i] for i in candidates]), spare
        for i in candidates:
            addition = min(reach - given[i], max(1, left * portions[i] // pool), spare)
            given[i] = given[i] + addition
            spare = spare - addition
    return np.array(given)


def bell_draw(stream_key, extent, spread, reach, split=(), held_as=jnp.bfloat16):
    values = spread * jax.random.normal(stream_key, extent, jnp.float32)
    if split:
        values = values * block_scale(stream_key, extent, split, -0.22, 0.18)
    return jnp.clip(values, -reach, reach).astype(held_as)


def setup_inputs(seed: int = 0) -> dict:
    seeds = jax.random.split(jax.random.key(seed), 8)
    inputs = bell_draw(seeds[0], (TOKENS, MODEL_WIDTH), 1.0, 6.0, ((0, 16), (1, 2)))
    cotangent = bell_draw(seeds[1], (TOKENS, MODEL_WIDTH), 1.0, 6.0, ((0, 16), (1, 2)))
    base_weight = bell_draw(seeds[2], (MODEL_WIDTH, MODEL_WIDTH), MODEL_WIDTH ** -0.5, 0.09375, ((1, 2),))
    adapter_ids_keys = jax.random.split(jax.random.fold_in(seeds[3], 1), TOKENS // TOK_DEV)
    adapter_ids_turns = jax.random.permutation(jax.random.fold_in(seeds[3], 3), TOKENS // TOK_DEV)
    adapter_ids = jax.vmap(lambda own, number: routed_block(jax.random.fold_in(seeds[3], 2), own, number, TOK_DEV, ADAPTERS, 1, MOST, 2))(adapter_ids_keys, adapter_ids_turns).reshape((TOKENS, 1))
    adapters = bell_draw(seeds[4], (ADAPTERS, 2, R, MODEL_WIDTH), MODEL_WIDTH ** -0.5, 0.09375, ((0, 16), (3, 2)), jnp.float32)
    first_moment = bell_draw(seeds[5], (ADAPTERS, 2, R, MODEL_WIDTH), 0.2, 3.0, ((0, 16), (3, 2)), jnp.float32)
    second_moment = jnp.clip(jnp.exp(math.log(1.0) - 2.9957323 * jax.random.uniform(seeds[6], (ADAPTERS, 2, R, MODEL_WIDTH), jnp.float32) ** block_scale(seeds[6], (ADAPTERS, 2, R, MODEL_WIDTH), ((0, 16), (3, 2)), -0.2, 0.2)), 0.05, 1.0)
    return dict(inputs=inputs, cotangent=cotangent, base_weight=base_weight, adapter_ids=adapter_ids, adapters=adapters, first_moment=first_moment, second_moment=second_moment)


adapter_scale = 2.0
beta_first = 0.9
beta_second = 0.999
adam_eps = 1e-08
learn_rate = 0.01
bias_first = 1.0 - math.exp(1000.0 * math.log(beta_first))
bias_second = 1.0 - math.exp(1000.0 * math.log(beta_second))

def adam_update(adapters, first_moment, second_moment, gradients, squares):
    clip_limit = math.sqrt(2.0 * R * MODEL_WIDTH)
    clip_factor = clip_limit / jnp.maximum(jnp.sqrt(squares), clip_limit)
    clipped = gradients * clip_factor[:, None, None, None]
    new_first = beta_first * first_moment + (1.0 - beta_first) * clipped
    new_second = beta_second * second_moment + (1.0 - beta_second) * clipped * clipped
    update = new_first / bias_first / (jnp.sqrt(new_second / bias_second) + adam_eps)
    return (adapters - learn_rate * update, new_first, new_second)

def adapter_grouped(pieces):
    incoming_rows, cotangent_rows, down_full, up_full = pieces
    down_reduced = down_full.astype(jnp.bfloat16)
    up_low = up_full.astype(jnp.bfloat16)
    projected = jnp.dot(incoming_rows, down_reduced.T, preferred_element_type=jnp.float32)
    pulled = jnp.dot(cotangent_rows, up_low.T, preferred_element_type=jnp.float32)
    projection_reduced = projected.astype(jnp.bfloat16)
    fetched_reduced = pulled.astype(jnp.bfloat16)
    down_gradient = adapter_scale * jnp.dot(fetched_reduced.T, incoming_rows, preferred_element_type=jnp.float32)
    up_gradient = adapter_scale * jnp.dot(projection_reduced.T, cotangent_rows, preferred_element_type=jnp.float32)
    adapter_rows = (adapter_scale * jnp.dot(fetched_reduced, down_reduced, preferred_element_type=jnp.float32)).astype(jnp.bfloat16)
    return (down_gradient, up_gradient, adapter_rows)

def reference(inputs, cotangent, base_weight, adapter_ids, adapters, first_moment, second_moment):
    chosen = adapter_ids[:, 0].astype(jnp.int32)
    blocks = chosen.reshape(N_AA, TOK_DEV)
    counter = jnp.arange(TOK_DEV, dtype=jnp.int32)
    matches = (blocks[:, :, None] == blocks[:, None, :]) & (counter[None, None, :] < counter[None, :, None])
    slot_rank = lax.optimization_barrier(jnp.sum(matches.astype(jnp.int32), axis=2))
    block_index = jnp.arange(N_AA, dtype=jnp.int32)[:, None]
    token_position = (blocks * (N_AA * MOST) + block_index * MOST + slot_rank).reshape(-1).astype(jnp.int32)
    slot_overall = ADAPTERS * N_AA * MOST
    incoming_rows = jnp.zeros((slot_overall, MODEL_WIDTH), jnp.bfloat16).at[token_position].set(inputs).reshape(ADAPTERS, N_AA * MOST, MODEL_WIDTH)
    cotangent_rows = jnp.zeros((slot_overall, MODEL_WIDTH), jnp.bfloat16).at[token_position].set(cotangent).reshape(ADAPTERS, N_AA * MOST, MODEL_WIDTH)
    down_gradient, up_gradient, adapter_rows = lax.map(adapter_grouped, (incoming_rows, cotangent_rows, adapters[:, 0], adapters[:, 1]))
    adapter_local = adapter_rows.reshape(slot_overall, MODEL_WIDTH)[token_position]
    frozen_term = jnp.dot(cotangent, base_weight.T, preferred_element_type=jnp.float32)
    input_gradient = (frozen_term + adapter_local.astype(jnp.float32)).astype(jnp.bfloat16)
    gradients = jnp.stack([down_gradient, up_gradient], axis=1)
    squares = lax.optimization_barrier(jnp.sum(gradients * gradients, axis=(1, 2, 3)))
    new_adapters, new_first, new_second = adam_update(adapters, first_moment, second_moment, gradients, squares)
    return (input_gradient, new_adapters, new_first, new_second, jnp.sqrt(jnp.sum(squares)))
```

```python
import functools
import math

import jax
import jax.numpy as jnp
from jax import lax
from jax.experimental import pallas as pl
from jax.experimental.pallas import tpu as pltpu
from jax.sharding import PartitionSpec as P

MODEL_WIDTH = 3584
R = 16


adapter_scale = 2.0
beta_first = 0.9
beta_second = 0.999
adam_eps = 1e-08
learn_rate = 0.01
bias_first = 1.0 - math.exp(1000.0 * math.log(beta_first))
bias_second = 1.0 - math.exp(1000.0 * math.log(beta_second))


def adam_update(adapters, first_moment, second_moment, gradients, squares):
    clip_limit = math.sqrt(2.0 * R * MODEL_WIDTH)
    clip_factor = clip_limit / jnp.maximum(jnp.sqrt(squares), clip_limit)
    clipped = gradients * clip_factor[:, None, None, None]
    new_first = beta_first * first_moment + (1.0 - beta_first) * clipped
    new_second = beta_second * second_moment + (1.0 - beta_second) * clipped * clipped
    update = new_first / bias_first / (jnp.sqrt(new_second / bias_second) + adam_eps)
    return (adapters - learn_rate * update, new_first, new_second)


def add_blocks(dst, src):
    lead, rows, _ = dst.shape
    step = 16

    def body(i, carry):
        a = i // (rows // step)
        r = pl.ds(pl.multiple_of((i % (rows // step)) * step, step), step)
        total = dst[a, r, :].astype(jnp.float32) + src[a, r, :].astype(jnp.float32)
        dst[a, r, :] = total.astype(dst.dtype)
        return carry

    lax.fori_loop(0, lead * (rows // step), body, 0)


class Line:
    def __init__(self, length, place, peer, block, ups, downs, sems):
        self.length, self.place, self.peer, self.block = length, place, peer, block
        self.ups, self.downs, self.sems = ups, downs, sems

    def copy(self, d, up):
        ways = self.ups if up else self.downs
        kind = 0 if up else 2
        return pltpu.make_async_remote_copy(
            src_ref=self.block(d),
            dst_ref=ways.at[d],
            send_sem=self.sems.at[kind, d],
            recv_sem=self.sems.at[kind + 1, d],
            device_id={"aa": self.peer(self.place + (1 if up else -1))},
            device_id_type=pl.DeviceIdType.MESH,
        )

    def step(self, d, up):
        p, last = self.place, self.length - 1
        ways = self.ups if up else self.downs

        @pl.when((p < d) if up else (p > d))
        def _():
            @pl.when((p > 0) if up else (p < last))
            def _():
                self.copy(d, up).wait_recv()
                add_blocks(self.block(d), ways.at[d])

            self.copy(d, up).start()

    def run(self):
        n = self.length

        @pl.when(self.place < n // 2)
        def _():
            for k in range(1, n):
                self.step(n - k, True)
                self.step(k - 1, False)

        @pl.when(self.place >= n // 2)
        def _():
            for k in range(1, n):
                self.step(k - 1, False)
                self.step(n - k, True)

    def arrive(self, use_up, use_down):
        p, last = self.place, self.length - 1

        @pl.when(p > 0)
        def _():
            self.copy(p, True).wait_recv()
            use_up(self.ups.at[p])

        @pl.when(p < last)
        def _():
            self.copy(p, False).wait_recv()
            use_down(self.downs.at[p])

    def drain(self):
        for d in range(self.length):
            @pl.when(self.place < d)
            def _():
                self.copy(d, True).wait_send()

            @pl.when(self.place > d)
            def _():
                self.copy(d, False).wait_send()


def scatter_kernel(
    outer, inner, down_ref, up_ref, out_ref, acc, ups_a, downs_a, ups_b, downs_b,
    ups_c, downs_c, ups_d, downs_d, core_sems, sems_a, sems_b, sems_c, sems_d,
):
    me = lax.axis_index("aa")
    core = me % 2
    y = (me // 2) % inner
    z = me // (2 * inner)
    index = lambda z, y, c: (z * inner + y) * 2 + c
    partner = index(z, y, 1 - core)
    along_y = lambda q: index(z, q, core)
    along_z = lambda q: index(q, y, core)
    barrier = pltpu.get_barrier_semaphore()

    def greet(device):
        pl.semaphore_signal(
            barrier, inc=1, device_id={"aa": device}, device_id_type=pl.DeviceIdType.MESH
        )

    greet(partner)
    for test, device in (
        (y > 0, along_y(y - 1)),
        (y < inner - 1, along_y(y + 1)),
        (z > 0, along_z(z - 1)),
        (z < outer - 1, along_z(z + 1)),
    ):
        @pl.when(test)
        def _():
            greet(device)

    one = lambda test: jnp.where(test, 1, 0)
    pl.semaphore_wait(
        barrier, 1 + one(y > 0) + one(y < inner - 1) + one(z > 0) + one(z < outer - 1)
    )
    swaps = []
    for h, ref in enumerate((down_ref, up_ref)):
        swaps.append(
            pltpu.make_async_remote_copy(
                src_ref=ref.at[:, :, 1 - core],
                dst_ref=acc.at[h],
                send_sem=core_sems.at[0, h],
                recv_sem=core_sems.at[1, h],
                device_id={"aa": partner},
                device_id_type=pl.DeviceIdType.MESH,
            )
        )
        swaps[-1].start()
    line_a = Line(inner, y, along_y, lambda d: acc.at[0, :, d], ups_a, downs_a, sems_a)
    line_b = Line(outer, z, along_z, lambda d: acc.at[1, d], ups_b, downs_b, sems_b)
    line_c = Line(outer, z, along_z, lambda d: acc.at[0, d, pl.ds(y, 1)], ups_c, downs_c, sems_c)
    line_d = Line(inner, y, along_y, lambda d: acc.at[1, z, pl.ds(d, 1)], ups_d, downs_d, sems_d)
    for h, (ref, line) in enumerate(((down_ref, line_a), (up_ref, line_b))):
        swaps[h].wait_recv()
        for a in range(outer):
            add_blocks(acc.at[h, a], ref.at[a, :, core])
        line.run()
    for line in (line_a, line_b):
        mine = line.block(line.place)
        line.arrive(functools.partial(add_blocks, mine), functools.partial(add_blocks, mine))
    line_c.run()
    line_d.run()
    rows = out_ref.shape[1]
    step = 16
    for h, line in ((1, line_d), (0, line_c)):
        own = line.block(line.place)

        @pl.loop(0, rows // step)
        def _(i):
            r = pl.ds(pl.multiple_of(i * step, step), step)
            out_ref[h, r, :] = own[0, r, :].astype(jnp.float32)

        def take(src):
            @pl.loop(0, rows // step)
            def _(i):
                r = pl.ds(pl.multiple_of(i * step, step), step)
                out_ref[h, r, :] += src[0, r, :].astype(jnp.float32)

        line.arrive(take, take)
    for swap in swaps:
        swap.wait_send()
    for line in (line_a, line_b, line_c, line_d):
        line.drain()


def reduce_scatter(down_gradient, up_gradient, owners):
    chips = owners // 2
    outer = 4 if chips % 4 == 0 else 1
    inner = chips // outer
    width = down_gradient.shape[-1]
    rows = down_gradient.shape[0] // owners
    shape = (outer, inner, 2, rows, width)
    buf = lambda *lead: pltpu.VMEM((*lead, rows, width), jnp.bfloat16)
    sem = lambda n: pltpu.SemaphoreType.DMA((4, n))
    return pl.pallas_call(
        functools.partial(scatter_kernel, outer, inner),
        out_shape=jax.ShapeDtypeStruct((2, rows, width), jnp.float32),
        in_specs=[pl.BlockSpec(memory_space=pltpu.VMEM)] * 2,
        out_specs=pl.BlockSpec(memory_space=pltpu.VMEM),
        scratch_shapes=[
            buf(2, outer, inner),
            buf(inner, outer), buf(inner, outer),
            buf(outer, inner), buf(outer, inner),
            buf(outer, 1), buf(outer, 1),
            buf(inner, 1), buf(inner, 1),
            pltpu.SemaphoreType.DMA((2, 2)),
            sem(inner), sem(outer), sem(outer), sem(inner),
        ],
        compiler_params=pltpu.CompilerParams(
            collective_id=0, has_side_effects=True, vmem_limit_bytes=60 * 1024 * 1024
        ),
        cost_estimate=pl.CostEstimate(
            flops=4 * down_gradient.size, bytes_accessed=40 * down_gradient.size, transcendentals=0
        ),
    )(down_gradient.reshape(shape), up_gradient.reshape(shape))


def local(inputs, cotangent, base_weight, adapter_ids, adapters, first_moment, second_moment):
    tok_rows, width = inputs.shape
    owners = lax.axis_size("aa")
    halves = lax.axis_size("ba")
    side = lax.axis_index("ba")
    local_count, _, rank, _ = adapters.shape
    total = owners * local_count
    dot = lambda a, b, dims: lax.dot_general(
        a, b, (dims, ((), ())), preferred_element_type=jnp.float32
    )
    low = adapters.astype(jnp.bfloat16)
    own = lambda k: low[:, k].reshape(local_count * rank, width)
    up = lax.all_gather(own(1), "aa", axis=0, tiled=True)
    down = lax.all_gather(own(0), "aa", axis=0, tiled=True)
    if halves == 2:
        swap = [(0, 1), (1, 0)]
        rows_of = lambda k: lax.dynamic_slice_in_dim(base_weight, k * width, width, axis=0)
        away = dot(cotangent, rows_of(1 - side), ((1,), (1,))).astype(jnp.bfloat16)
        away = lax.ppermute(away, "ba", swap)
        frozen_term = dot(cotangent, rows_of(side), ((1,), (1,)))
        both = lambda a: a + lax.ppermute(a, "ba", swap)
    else:
        partial_sums = dot(cotangent, base_weight, ((1,), (1,)))
        frozen_term = lax.psum_scatter(partial_sums, "ba", scatter_dimension=1, tiled=True)
        away = jnp.zeros((), jnp.bfloat16)
        both = lambda a: lax.psum(a, "ba")
    mine = adapter_ids == (jnp.arange(total * rank, dtype=jnp.int32) // rank)[None, :]
    pulled = jnp.where(mine, dot(cotangent, up, ((1,), (1,))), 0.0)
    projected = jnp.where(mine, dot(inputs, down, ((1,), (1,))), 0.0)
    fold = lambda a: a.reshape(tok_rows, total * rank // 128, 128).sum(axis=1)
    fold2 = lambda a: fold(a).reshape(tok_rows, 128 // rank, rank).sum(axis=1)
    small = both(jnp.concatenate([fold2(projected), fold2(pulled)], axis=1)).astype(jnp.bfloat16)
    spread = lambda a: jnp.where(mine, jnp.tile(a, (1, total)), jnp.bfloat16(0))
    proj_low = spread(small[:, :rank])
    pull_low = spread(small[:, rank:])
    grad = lambda a, b: (adapter_scale * dot(a, b, ((0,), (0,)))).astype(jnp.bfloat16)
    down_gradient = grad(pull_low, inputs)
    up_gradient = grad(proj_low, cotangent)
    lora_part = (adapter_scale * dot(pull_low, down, ((1,), (0,)))).astype(jnp.bfloat16)
    summed = reduce_scatter(down_gradient, up_gradient, owners)
    input_gradient = (
        frozen_term + away.astype(jnp.float32) + lora_part.astype(jnp.float32)
    ).astype(jnp.bfloat16)
    gradients = jnp.stack(
        [summed[k].reshape(local_count, rank, width) for k in range(2)], axis=1
    )
    part_squares = jnp.sum(gradients * gradients, axis=(1, 2, 3))
    every = lax.all_gather(part_squares, ("aa", "ba")).reshape(owners, halves, local_count)
    squares = lax.dynamic_index_in_dim(every, lax.axis_index("aa"), 0, False).sum(axis=0)
    new_adapters, new_first, new_second = adam_update(
        adapters, first_moment, second_moment, gradients, squares
    )
    return (input_gradient, new_adapters, new_first, new_second, jnp.sqrt(jnp.sum(every)))


def solution(mesh):
    in_specs = (
        P("aa", "ba"),
        P("aa", "ba"),
        P(None, "ba"),
        P("aa", None),
        P("aa", None, None, "ba"),
        P("aa", None, None, "ba"),
        P("aa", None, None, "ba"),
    )
    out_specs = (
        P("aa", "ba"),
        P("aa", None, None, "ba"),
        P("aa", None, None, "ba"),
        P("aa", None, None, "ba"),
        P(),
    )
    return jax.shard_map(local, mesh=mesh, in_specs=in_specs, out_specs=out_specs, check_vma=False)
```

```python
import functools
import math

import jax
import jax.numpy as jnp
from jax import lax
from jax.experimental import pallas as pl
from jax.experimental.pallas import tpu as pltpu
from jax.sharding import PartitionSpec as P

MODEL_WIDTH = 3584
R = 16


adapter_scale = 2.0
beta_first = 0.9
beta_second = 0.999
adam_eps = 1e-08
learn_rate = 0.01
bias_first = 1.0 - math.exp(1000.0 * math.log(beta_first))
bias_second = 1.0 - math.exp(1000.0 * math.log(beta_second))


def adam_update(adapters, first_moment, second_moment, gradients, squares):
    clip_limit = math.sqrt(2.0 * R * MODEL_WIDTH)
    clip_factor = clip_limit / jnp.maximum(jnp.sqrt(squares), clip_limit)
    clipped = gradients * clip_factor[:, None, None, None]
    new_first = beta_first * first_moment + (1.0 - beta_first) * clipped
    new_second = beta_second * second_moment + (1.0 - beta_second) * clipped * clipped
    update = new_first / bias_first / (jnp.sqrt(new_second / bias_second) + adam_eps)
    return (adapters - learn_rate * update, new_first, new_second)


def add_blocks(dst, src):
    lead, rows, _ = dst.shape
    step = 16

    def body(i, carry):
        a = i // (rows // step)
        r = pl.ds(pl.multiple_of((i % (rows // step)) * step, step), step)
        total = dst[a, r, :].astype(jnp.float32) + src[a, r, :].astype(jnp.float32)
        dst[a, r, :] = total.astype(dst.dtype)
        return carry

    lax.fori_loop(0, lead * (rows // step), body, 0)


class Line:
    def __init__(self, length, place, peer, block, ups, downs, sems):
        self.length, self.place, self.peer, self.block = length, place, peer, block
        self.ups, self.downs, self.sems = ups, downs, sems

    def copy(self, d, up):
        ways = self.ups if up else self.downs
        kind = 0 if up else 2
        return pltpu.make_async_remote_copy(
            src_ref=self.block(d),
            dst_ref=ways.at[d],
            send_sem=self.sems.at[kind, d],
            recv_sem=self.sems.at[kind + 1, d],
            device_id={"aa": self.peer(self.place + (1 if up else -1))},
            device_id_type=pl.DeviceIdType.MESH,
        )

    def step(self, d, up):
        p, last = self.place, self.length - 1
        ways = self.ups if up else self.downs

        @pl.when((p < d) if up else (p > d))
        def _():
            @pl.when((p > 0) if up else (p < last))
            def _():
                self.copy(d, up).wait_recv()
                add_blocks(self.block(d), ways.at[d])

            self.copy(d, up).start()

    def run(self):
        n = self.length

        @pl.when(self.place < n // 2)
        def _():
            for k in range(1, n):
                self.step(n - k, True)
                self.step(k - 1, False)

        @pl.when(self.place >= n // 2)
        def _():
            for k in range(1, n):
                self.step(k - 1, False)
                self.step(n - k, True)

    def arrive(self, use_up, use_down):
        p, last = self.place, self.length - 1

        @pl.when(p > 0)
        def _():
            self.copy(p, True).wait_recv()
            use_up(self.ups.at[p])

        @pl.when(p < last)
        def _():
            self.copy(p, False).wait_recv()
            use_down(self.downs.at[p])

    def drain(self):
        for d in range(self.length):
            @pl.when(self.place < d)
            def _():
                self.copy(d, True).wait_send()

            @pl.when(self.place > d)
            def _():
                self.copy(d, False).wait_send()


def scatter_kernel(
    outer, inner, down_ref, up_ref, out_ref, acc, ups_a, downs_a, ups_b, downs_b,
    ups_c, downs_c, ups_d, downs_d, core_sems, sems_a, sems_b, sems_c, sems_d,
):
    me = lax.axis_index("aa")
    core = me % 2
    y = (me // 2) % inner
    z = me // (2 * inner)
    index = lambda z, y, c: (z * inner + y) * 2 + c
    partner = index(z, y, 1 - core)
    along_y = lambda q: index(z, q, core)
    along_z = lambda q: index(q, y, core)
    barrier = pltpu.get_barrier_semaphore()

    def greet(device):
        pl.semaphore_signal(
            barrier, inc=1, device_id={"aa": device}, device_id_type=pl.DeviceIdType.MESH
        )

    greet(partner)
    for test, device in (
        (y > 0, along_y(y - 1)),
        (y < inner - 1, along_y(y + 1)),
        (z > 0, along_z(z - 1)),
        (z < outer - 1, along_z(z + 1)),
    ):
        @pl.when(test)
        def _():
            greet(device)

    one = lambda test: jnp.where(test, 1, 0)
    pl.semaphore_wait(
        barrier, 1 + one(y > 0) + one(y < inner - 1) + one(z > 0) + one(z < outer - 1)
    )
    swaps = []
    for h, ref in enumerate((down_ref, up_ref)):
        swaps.append(
            pltpu.make_async_remote_copy(
                src_ref=ref.at[:, :, 1 - core],
                dst_ref=acc.at[h],
                send_sem=core_sems.at[0, h],
                recv_sem=core_sems.at[1, h],
                device_id={"aa": partner},
                device_id_type=pl.DeviceIdType.MESH,
            )
        )
        swaps[-1].start()
    line_a = Line(inner, y, along_y, lambda d: acc.at[0, :, d], ups_a, downs_a, sems_a)
    line_b = Line(outer, z, along_z, lambda d: acc.at[1, d], ups_b, downs_b, sems_b)
    line_c = Line(outer, z, along_z, lambda d: acc.at[0, d, pl.ds(y, 1)], ups_c, downs_c, sems_c)
    line_d = Line(inner, y, along_y, lambda d: acc.at[1, z, pl.ds(d, 1)], ups_d, downs_d, sems_d)
    for h, (ref, line) in enumerate(((down_ref, line_a), (up_ref, line_b))):
        swaps[h].wait_recv()
        for a in range(outer):
            add_blocks(acc.at[h, a], ref.at[a, :, core])
        line.run()
    for line in (line_a, line_b):
        mine = line.block(line.place)
        line.arrive(functools.partial(add_blocks, mine), functools.partial(add_blocks, mine))
    line_c.run()
    line_d.run()
    rows = out_ref.shape[1]
    step = 16
    for h, line in ((1, line_d), (0, line_c)):
        own = line.block(line.place)

        @pl.loop(0, rows // step)
        def _(i):
            r = pl.ds(pl.multiple_of(i * step, step), step)
            out_ref[h, r, :] = own[0, r, :].astype(jnp.float32)

        def take(src):
            @pl.loop(0, rows // step)
            def _(i):
                r = pl.ds(pl.multiple_of(i * step, step), step)
                out_ref[h, r, :] += src[0, r, :].astype(jnp.float32)

        line.arrive(take, take)
    for swap in swaps:
        swap.wait_send()
    for line in (line_a, line_b, line_c, line_d):
        line.drain()


def reduce_scatter(down_gradient, up_gradient, owners):
    chips = owners // 2
    outer = 4 if chips % 4 == 0 else 1
    inner = chips // outer
    width = down_gradient.shape[-1]
    rows = down_gradient.shape[0] // owners
    shape = (outer, inner, 2, rows, width)
    buf = lambda *lead: pltpu.VMEM((*lead, rows, width), jnp.bfloat16)
    sem = lambda n: pltpu.SemaphoreType.DMA((4, n))
    return pl.pallas_call(
        functools.partial(scatter_kernel, outer, inner),
        out_shape=jax.ShapeDtypeStruct((2, rows, width), jnp.float32),
        in_specs=[pl.BlockSpec(memory_space=pltpu.VMEM)] * 2,
        out_specs=pl.BlockSpec(memory_space=pltpu.VMEM),
        scratch_shapes=[
            buf(2, outer, inner),
            buf(inner, outer), buf(inner, outer),
            buf(outer, inner), buf(outer, inner),
            buf(outer, 1), buf(outer, 1),
            buf(inner, 1), buf(inner, 1),
            pltpu.SemaphoreType.DMA((2, 2)),
            sem(inner), sem(outer), sem(outer), sem(inner),
        ],
        compiler_params=pltpu.CompilerParams(
            collective_id=0, has_side_effects=True, vmem_limit_bytes=60 * 1024 * 1024
        ),
        cost_estimate=pl.CostEstimate(
            flops=4 * down_gradient.size, bytes_accessed=40 * down_gradient.size, transcendentals=0
        ),
    )(down_gradient.reshape(shape), up_gradient.reshape(shape))


def local(inputs, cotangent, base_weight, adapter_ids, adapters, first_moment, second_moment):
    tok_rows, width = inputs.shape
    owners = lax.axis_size("aa")
    halves = lax.axis_size("ba")
    side = lax.axis_index("ba")
    local_count, _, rank, _ = adapters.shape
    total = owners * local_count
    dot = lambda a, b, dims: lax.dot_general(
        a, b, (dims, ((), ())), preferred_element_type=jnp.float32
    )
    low = adapters.astype(jnp.bfloat16)
    own = lambda k: low[:, k].reshape(local_count * rank, width)
    up = lax.all_gather(own(1), "aa", axis=0, tiled=True)
    down = lax.all_gather(own(0), "aa", axis=0, tiled=True)
    if halves == 2:
        swap = [(0, 1), (1, 0)]
        rows_of = lambda k: lax.dynamic_slice_in_dim(base_weight, k * width, width, axis=0)
        away = dot(cotangent, rows_of(1 - side), ((1,), (1,))).astype(jnp.bfloat16)
        cot_away, away = lax.optimization_barrier((cotangent, away))
        away = lax.ppermute(away, "ba", swap)
        frozen_term = dot(cot_away, rows_of(side), ((1,), (1,)))
        both = lambda a: a + lax.ppermute(a, "ba", swap)
    else:
        partial_sums = dot(cotangent, base_weight, ((1,), (1,)))
        frozen_term = lax.psum_scatter(partial_sums, "ba", scatter_dimension=1, tiled=True)
        away = jnp.zeros((), jnp.bfloat16)
        both = lambda a: lax.psum(a, "ba")
    cot_after, frozen_term = lax.optimization_barrier((cotangent, frozen_term))
    mine = adapter_ids == (jnp.arange(total * rank, dtype=jnp.int32) // rank)[None, :]
    pulled = jnp.where(mine, dot(cot_after, up, ((1,), (1,))), 0.0)
    projected = jnp.where(mine, dot(inputs, down, ((1,), (1,))), 0.0)
    fold = lambda a: a.reshape(tok_rows, total * rank // 128, 128).sum(axis=1)
    fold2 = lambda a: fold(a).reshape(tok_rows, 128 // rank, rank).sum(axis=1)
    small = both(jnp.concatenate([fold2(projected), fold2(pulled)], axis=1)).astype(jnp.bfloat16)
    spread = lambda a: jnp.where(mine, jnp.tile(a, (1, total)), jnp.bfloat16(0))
    proj_low = spread(small[:, :rank])
    pull_low = spread(small[:, rank:])
    grad = lambda a, b: (adapter_scale * dot(a, b, ((0,), (0,)))).astype(jnp.bfloat16)
    down_gradient = grad(pull_low, inputs)
    up_gradient = grad(proj_low, cotangent)
    lora_part = (adapter_scale * dot(pull_low, down, ((1,), (0,)))).astype(jnp.bfloat16)
    summed = reduce_scatter(down_gradient, up_gradient, owners)
    input_gradient = (
        frozen_term + away.astype(jnp.float32) + lora_part.astype(jnp.float32)
    ).astype(jnp.bfloat16)
    gradients = jnp.stack(
        [summed[k].reshape(local_count, rank, width) for k in range(2)], axis=1
    )
    part_squares = jnp.sum(gradients * gradients, axis=(1, 2, 3))
    squares = both(part_squares)
    grand_total = jnp.sum(squares)
    if owners & (owners - 1) == 0:
        stride = 1
        while stride < owners:
            pairs = [(k, k ^ stride) for k in range(owners)]
            grand_total = grand_total + lax.ppermute(grand_total, "aa", pairs)
            stride *= 2
    else:
        grand_total = lax.psum(grand_total, "aa")
    new_adapters, new_first, new_second = adam_update(
        adapters, first_moment, second_moment, gradients, squares
    )
    return (input_gradient, new_adapters, new_first, new_second, jnp.sqrt(grand_total))


def solution(mesh):
    in_specs = (
        P("aa", "ba"),
        P("aa", "ba"),
        P(None, "ba"),
        P("aa", None),
        P("aa", None, None, "ba"),
        P("aa", None, None, "ba"),
        P("aa", None, None, "ba"),
    )
    out_specs = (
        P("aa", "ba"),
        P("aa", None, None, "ba"),
        P("aa", None, None, "ba"),
        P("aa", None, None, "ba"),
        P(),
    )
    return jax.shard_map(local, mesh=mesh, in_specs=in_specs, out_specs=out_specs, check_vma=False)
```
